32 devices in a mesh: event: 4 (over z), slab: 8 (over y, x, core).
Axes of the slice: x: 2, y: 2, z: 4, core: 2. Of those that a mesh axis runs over, the one named last changes fastest.
Arguments:
- wave_prev: float32 [4, 256, 128, 128], P('event', 'slab'), may hold values from -6 to 6
- wave_now: float32 [4, 256, 128, 128], P('event', 'slab'), may hold values from -6 to 6
- adjoint: float32 [4, 4, 256, 128, 128], P('event', None, 'slab'), may hold values from -6 to 6
- background: float32 [4, 256, 128, 128], P('event', 'slab'), may hold values from 0.02 to 0.12
- coeffs_x: float32 [4, 256, 9], P('event', 'slab'), may hold values from -2 to 2
- stiff_y: float32 [128, 128], replicated, may hold values from -0.5 to 0.5
- stiff_z: float32 [128, 128], replicated, may hold values from -0.5 to 0.5
- interp_y: bfloat16 [16, 32], replicated, may hold values from -1.5 to 1.5
- interp_z: bfloat16 [128, 128], replicated, may hold values from -0.5 to 0.5
- model: bfloat16 [1024, 16, 128], P(('event', 'slab')), may hold values from -1.796875 to 1.796875
- block_index: int32 [4, 256, 4], P('event', 'slab'), may hold values from 0 to 1023, as said below
- live_count: int32 [4, 8], P('event', 'slab'), may hold values from 1 to 128, as said below
Outputs:
- wave_last: float32 [4, 256, 128, 128], P('event', 'slab')
- model_gradient: float32 [1024, 16, 128], P(('event', 'slab'))
The draws below stay inside these ranges and needn't reach their ends.
Inputs may be any that keep to these rules, and one draw needn't show every extreme that they name: `block_index`: within one slab of one event, at most 8 tiles name blocks owned by one device, and some device owns exactly 8 of them. `live_count`: some slab has all 128 tiles live.
All inputs are finite; a program needn't handle non-finite values.
Results may differ from the reference program's by a relative error of at most 0.0029.
Values may be sent and summed in bfloat16 or wider, within the bound.
No kernel may reach another device: no remote copies, remote signals or barrier semaphores. Data moves between devices by JAX's collectives and lax.ppermute only.
A program may use at most 128 MiB of HBM per device.

```python
import math
import jax
import jax.numpy as jnp
from jax import lax

PL = 32
NY = 128
NZ = 128
REACH = 4
STEPS = 4
QY = 4
BY = 16
BZ = 128
EVENTS = 4
NX = 256
TY = 32
CAP = 8
BLK_DEV = 32
MB = 1024
N_EVENT = 4
N_SLAB = 8
DEVICES = 32


def draw_block_index(key, part):
    n_tiles = PL * QY
    subkeys = jax.random.split(jax.random.fold_in(key, 11), N_EVENT * N_SLAB)

    def one_slab(slab_key):
        first_key, second_key, third_key, fourth_key = jax.random.split(slab_key, 4)
        shuffled = jax.random.permutation(first_key, DEVICES)
        others = jax.random.permutation(second_key, (DEVICES - 1) * CAP)[:n_tiles - CAP]
        chosen = jnp.concatenate([jnp.zeros((CAP,), jnp.int32), (1 + others // CAP).astype(jnp.int32)])
        owners = shuffled[chosen]
        owners = owners[jax.random.permutation(third_key, n_tiles)]
        local_ids = jax.random.randint(fourth_key, (n_tiles,), 0, BLK_DEV)
        return (owners * BLK_DEV + local_ids).astype(jnp.int32)
    block_ids = jax.vmap(one_slab)(subkeys)
    return block_ids.reshape(N_EVENT, N_SLAB * PL, QY)


def draw_live_count(key, part):
    first_key, second_key = jax.random.split(jax.random.fold_in(key, 23))
    counts = jax.random.randint(first_key, (N_EVENT * N_SLAB,), 1, PL * QY + 1)
    full_dev = jax.random.randint(second_key, (), 0, N_EVENT * N_SLAB)
    counts = jnp.where(jnp.arange(N_EVENT * N_SLAB) == full_dev, PL * QY, counts)
    return counts.reshape(N_EVENT, N_SLAB).astype(jnp.int32)


def level_of(rng, extent, shards, least, largest):
    def one(axis_at, parts):
        steps = jax.random.uniform(jax.random.fold_in(jax.random.fold_in(rng, 6), axis_at), (parts,), jnp.float32, least / len(shards), largest / len(shards))
        return jnp.repeat(jnp.exp(steps), extent[axis_at] // parts).reshape((-1,) + (1,) * (len(extent) - axis_at - 1))

    factor_of = one(*shards[0])
    for cut in shards[1:]:
        factor_of = factor_of * one(*cut)
    return factor_of


def noise(key, extent, spread, most, cuts=(), kind=jnp.bfloat16):
    drawn = jax.random.normal(key, extent, jnp.float32) * spread
    if len(cuts) > 0:
        drawn = level_of(key, extent, cuts, -0.22, 0.18) * drawn
    return jnp.clip(drawn, min=-most, max=most).astype(kind)


def setup_inputs(seed: int = 0) -> dict:
    arg_keys = jax.random.split(jax.random.key(seed), 13)
    wave_prev = noise(arg_keys[0], (EVENTS, NX, NY, NZ), 1.0, 6.0, ((0, 4), (1, 8)), jnp.float32)
    wave_now = noise(arg_keys[1], (EVENTS, NX, NY, NZ), 1.0, 6.0, ((0, 4), (1, 8)), jnp.float32)
    adjoint = noise(arg_keys[2], (EVENTS, STEPS, NX, NY, NZ), 1.0, 6.0, ((0, 4), (2, 8)), jnp.float32)
    background = jnp.clip(jnp.exp(math.log(0.12) - 1.7917595 * jax.random.uniform(arg_keys[3], (EVENTS, NX, NY, NZ), jnp.float32) ** level_of(arg_keys[3], (EVENTS, NX, NY, NZ), ((0, 4), (1, 8)), -0.2, 0.2)), 0.02, 0.12)
    coeffs_x = noise(arg_keys[4], (EVENTS, NX, 2 * REACH + 1), (2 * REACH + 1) ** -0.5, 2.0, ((0, 4), (1, 8)), jnp.float32)
    stiff_y = noise(arg_keys[5], (NY, NY), NY ** -0.5, 0.5, (), jnp.float32)
    stiff_z = noise(arg_keys[6], (NZ, NZ), NZ ** -0.5, 0.5, (), jnp.float32)
    interp_y = noise(arg_keys[7], (BY, TY), BY ** -0.5, 1.5)
    interp_z = noise(arg_keys[8], (BZ, NZ), BZ ** -0.5, 0.5)
    model = noise(arg_keys[9], (MB, BY, BZ), 0.3, 1.796875, ((0, 32),))
    block_index = draw_block_index(jax.random.fold_in(arg_keys[12], 71), 0)
    live_count = draw_live_count(jax.random.fold_in(arg_keys[12], 71), 0)
    return dict(wave_prev=wave_prev, wave_now=wave_now, adjoint=adjoint, background=background, coeffs_x=coeffs_x, stiff_y=stiff_y, stiff_z=stiff_z, interp_y=interp_y, interp_z=interp_z, model=model, block_index=block_index, live_count=live_count)


HIGH = lax.Precision.HIGHEST


def stiffness(wavefield, coeffs, stiff_y, stiff_z):
    half_width = (coeffs.shape[-1] - 1) // 2
    n_planes = wavefield.shape[0]
    padded = jnp.pad(wavefield, ((half_width, half_width), (0, 0), (0, 0)))
    result = jnp.einsum("yw,xwz->xyz", stiff_y, wavefield, precision=HIGH)
    result = result + jnp.einsum("xyw,zw->xyz", wavefield, stiff_z, precision=HIGH)
    for offset in range(2 * half_width + 1):
        result = result + coeffs[:, offset][:, None, None] * padded[offset:offset + n_planes]
    return result


def interpolate(blocks, interp_y, interp_z):
    n_tiles = blocks.shape[0]
    along_z = jnp.dot(blocks.reshape(-1, blocks.shape[2]), interp_z, preferred_element_type=jnp.float32)
    along_z = along_z.reshape(n_tiles, blocks.shape[1], -1)
    return jnp.einsum("by,tbz->tyz", interp_y.astype(jnp.float32), along_z, precision=HIGH)


def transpose_interp(kernel_low, interp_y, interp_z, n_tiles):
    rows_tile = interp_y.shape[1]
    back_z = jnp.dot(kernel_low.reshape(-1, kernel_low.shape[2]), interp_z.T, preferred_element_type=jnp.float32)
    back_z = back_z.reshape(n_tiles, rows_tile, -1)
    return jnp.einsum("by,tyc->tbc", interp_y.astype(jnp.float32), back_z, precision=HIGH)


def reference(wave_prev, wave_now, adjoint, background, coeffs_x, stiff_y, stiff_z, interp_y, interp_z, model, block_index, live_count):
    def one_event(inputs):
        prev_w, now_w, adj_w, back_w, coeffs, block_ids, counts = inputs
        n_planes = now_w.shape[0]
        per_slab = n_planes // N_SLAB
        blocks = model[block_ids.reshape(-1)]
        perturb = interpolate(blocks, interp_y, interp_z).reshape(n_planes, NY, NZ)
        tile_num = (jnp.arange(n_planes, dtype=jnp.int32) % per_slab)[:, None] * QY + jnp.arange(QY, dtype=jnp.int32)[None, :]
        slab_of = jnp.arange(n_planes, dtype=jnp.int32) // per_slab
        alive = tile_num < counts[slab_of][:, None]
        alive_rows = jnp.repeat(alive, TY, axis=1)[:, :, None]
        speed_sq = back_w * jnp.exp(jnp.where(alive_rows, perturb, jnp.zeros_like(perturb)))
        kernel = jnp.zeros_like(now_w)
        for time_step in range(STEPS):
            stiff_u = stiffness(now_w, coeffs, stiff_y, stiff_z)
            kernel = kernel - adj_w[time_step] * speed_sq * stiff_u
            prev_w, now_w = now_w, 2.0 * now_w - prev_w - speed_sq * stiff_u
        gradients = transpose_interp(kernel.astype(jnp.bfloat16), interp_y, interp_z, n_planes * QY)
        gradients = gradients * alive.reshape(-1)[:, None, None].astype(gradients.dtype)
        return now_w, gradients

    wave_last, gradients = lax.map(one_event, (wave_prev, wave_now, adjoint, background, coeffs_x, block_index, live_count))
    n_blocks = model.shape[0]
    summed = jax.ops.segment_sum(gradients.reshape(-1, BY * BZ), block_index.reshape(-1), num_segments=n_blocks)
    return wave_last, summed.reshape(n_blocks, BY, BZ)
```

```python
import functools

import jax
import jax.numpy as jnp
from jax import lax
from jax.experimental import pallas as pl
from jax.experimental.pallas import tpu as pltpu
from jax.sharding import PartitionSpec as P

F32 = jnp.float32
BF16 = jnp.bfloat16
I32 = jnp.int32
VM = pltpu.VMEM
ROWS = 32


def vspec():
    return pl.BlockSpec(memory_space=pltpu.VMEM)


def sspec():
    return pl.BlockSpec(memory_space=pltpu.SMEM)


def aspec():
    return pl.BlockSpec(memory_space=pl.ANY)


def in_vmem(x):
    return pltpu.with_memory_space_constraint(x, pltpu.VMEM)


def hbm(x):
    return pltpu.with_memory_space_constraint(x, pltpu.HBM)


def split2(value):
    high = value.astype(BF16)
    low = (value - high.astype(F32)).astype(BF16)
    return high, low


def split2_outside(value):
    rounded = lax.reduce_precision(value, exponent_bits=8, mantissa_bits=7)
    return rounded.astype(BF16), (value - rounded).astype(BF16)


def call(body, args, specs, outs, scratch=(), aliases=None, mib=24, name=None, out_specs=None):
    return pl.pallas_call(
        body,
        out_shape=outs,
        in_specs=specs,
        out_specs=out_specs or [vspec() for _ in outs],
        scratch_shapes=list(scratch),
        input_output_aliases=aliases or {},
        compiler_params=pltpu.CompilerParams(vmem_limit_bytes=mib * 1024 * 1024),
        name=name,
    )(*args)


def stiff_group(tap, first, width, reach, coef, wz, ly, part, emit):
    taps = 2 * reach + 1
    ny = part.shape[1]
    nz = part.shape[2]
    every = slice(0, ny)
    for j in range(0, width, 2):
        ah, al = split2(tap(reach + j)(every))
        bh, bl = split2(tap(reach + j + 1)(every))
        left = jnp.concatenate(
            [jnp.concatenate([ah, al], axis=1), jnp.concatenate([bh, bl], axis=1)], axis=0
        )
        rz = jnp.dot(left, wz[...], preferred_element_type=F32)
        right = jnp.concatenate(
            [jnp.concatenate([ah, bh], axis=1), jnp.concatenate([al, bl], axis=1)], axis=0
        )
        ry = jnp.dot(ly[...], right, preferred_element_type=F32)
        part[j] = (rz[:ny, :nz] + rz[:ny, nz:]) + (ry[:ny, :nz] + ry[ny:, :nz])
        part[j + 1] = (rz[ny:, :nz] + rz[ny:, nz:]) + (ry[:ny, nz:] + ry[ny:, nz:])
    for j in range(width):
        weights = [coef[(first + j) * taps + k] for k in range(taps)]
        for row in range(0, ny, ROWS):
            rows = slice(row, row + ROWS)
            total = part[j, rows]
            for k in range(taps):
                total = total + weights[k] * tap(j + k)(rows)
            emit(j, rows, total)


def first_body(reach, steps, *refs):
    wave, before, back, adjoint, below, above, coef, wz, ly = refs[:9]
    refs = refs[12:]
    stiff, ahead, now, background = refs[:4]
    adj = refs[4 : 4 + steps]
    prev, halo, part, sems = refs[4 + steps :]
    n = now.shape[0]
    pairs = [(wave.at[0], now), (before.at[0], prev), (back.at[0], background)]
    pairs += [(adjoint.at[0, s], adj[s]) for s in range(steps)]
    copies = [pltpu.make_async_copy(src, dst, sems.at[i]) for i, (src, dst) in enumerate(pairs)]
    for copy in copies:
        copy.start()
    halo[0:reach] = below[...].astype(F32)
    halo[reach : 2 * reach] = above[...].astype(F32)
    copies[0].wait()
    copies[1].wait()

    def group(first, tap):
        def emit(j, rows, value):
            stiff[first + j, rows] = value
            here = now[first + j, rows]
            ahead[first + j, rows] = (here + here) - prev[first + j, rows]

        stiff_group(tap, first, reach, reach, coef, wz, ly, part, emit)

    def step(g, carry):
        first = (g + 1) * reach
        group(first, lambda j: lambda rows: now[first - reach + j, rows])
        return carry

    lax.fori_loop(0, n // reach - 2, step, 0)
    for first in (0, n - reach):
        group(first, edge_tap(now, halo, first, reach))
    for copy in copies[2:]:
        copy.wait()


def edge_tap(now, halo, first, reach):
    n = now.shape[0]

    def tap(j):
        x = first - reach + j
        if x < 0:
            return lambda rows: halo[j, rows]
        if x >= n:
            return lambda rows: halo[reach + x - n, rows]
        return lambda rows: now[x, rows]

    return tap


def start_body(reach, slabs, *refs):
    fetched, refs = refs[:slabs], refs[slabs:]
    slot, live, iz, spread, background, ahead, stiff, adj = refs[:8]
    speed, nxt, kern, low_out, high_out, table, blocks, along = refs[8:]
    n, ny, nz = background.shape
    tiles = slot.shape[0]
    per_plane = tiles // n
    by = table.shape[1]
    rows_plane = per_plane * by
    alive = live[0]
    zero = jnp.zeros(table.shape[1:], BF16)
    count = fetched[0].shape[0]
    for r, piece in enumerate(fetched):
        table[r * count : (r + 1) * count] = piece[...]

    def place(t, carry):
        block = table[slot[t]]
        blocks[pl.ds(pl.multiple_of(t * by, by), by)] = jnp.where(t < alive, block, zero)
        return carry

    lax.fori_loop(0, tiles, place, 0, unroll=8)
    chunk = 8 * rows_plane

    def wide(i, carry):
        at = pl.ds(pl.multiple_of(i * chunk, chunk), chunk)
        along[at] = jnp.dot(blocks[at], iz[...], preferred_element_type=F32)
        return carry

    lax.fori_loop(0, n // 8, wide, 0)

    def pair(g, carry):
        cols = []
        for j in range(2):
            at = pl.multiple_of((2 * g + j) * rows_plane, rows_plane)
            high, low = split2(along[pl.ds(at, rows_plane)])
            cols.append(jnp.concatenate([high, low], axis=0))
        perturb = jnp.dot(spread[...], jnp.concatenate(cols, axis=1), preferred_element_type=F32)
        for j in range(2):
            x = 2 * g + j
            c = background[x] * jnp.exp(perturb[:, j * nz : (j + 1) * nz])
            speed[x] = c
            push = c * stiff[x]
            nxt[x] = ahead[x] - push
            kern[x] = -(adj[x] * push)
        return carry

    lax.fori_loop(0, n // 2, pair, 0, unroll=2)
    low_out[...] = nxt[0:reach].astype(BF16)
    high_out[...] = nxt[n - reach : n].astype(BF16)


def tile_gradients(kern_plane, izt, collect, width, put):
    for j in range(0, width, 2):
        cols = []
        for i in (j, j + 1):
            back = jnp.dot(kern_plane(i).astype(BF16), izt[...], preferred_element_type=F32)
            high, low = split2(back)
            cols.append(jnp.concatenate([high, low], axis=0))
        grads = jnp.dot(collect[...], jnp.concatenate(cols, axis=1), preferred_element_type=F32)
        half = grads.shape[1] // 2
        put(j, grads[:, :half].astype(BF16))
        put(j + 1, grads[:, half:].astype(BF16))


def inner_body(reach, last, now, prev, speed, kern, adj, coef, wz, ly, *rest):
    if last:
        izt, collect, nxt, kern_out, inner, part = rest
    else:
        nxt, kern_out, part = rest
    n = now.shape[0]

    def step(g, carry):
        first = (g + 1) * reach

        def tap(j):
            return lambda rows: now[first - reach + j, rows]

        def emit(j, rows, value):
            x = first + j
            push = speed[x, rows] * value
            kern_out[x, rows] = kern[x, rows] - adj[x, rows] * push
            here = now[x, rows]
            nxt[x, rows] = ((here + here) - prev[x, rows]) - push

        stiff_group(tap, first, reach, reach, coef, wz, ly, part, emit)
        if last:
            rows_plane = collect.shape[0]

            def put(j, value):
                at = pl.multiple_of((g * reach + j) * rows_plane, rows_plane)
                inner[pl.ds(at, rows_plane)] = value

            tile_gradients(lambda j: kern_out[first + j], izt, collect, reach, put)
        return carry

    lax.fori_loop(0, n // reach - 2, step, 0)


def outer_body(reach, last, now, prev, speed, kern, adj, below, above, coef, wz, ly, *rest):
    if last:
        izt, collect, inner, slot, live, nxt, kern_out, outgoing, wave, part, halo, edge, sems = rest
    else:
        nxt, kern_out, low_out, high_out, part, halo = rest
    n = now.shape[0]
    if last:
        copies = [
            pltpu.make_async_copy(nxt.at[pl.ds(at, count)], wave.at[0, pl.ds(at, count)], sems.at[i])
            for i, (at, count) in enumerate([(reach, n - 2 * reach), (0, reach), (n - reach, reach)])
        ]
        copies[0].start()
    halo[0:reach] = below[...].astype(F32)
    halo[reach : 2 * reach] = above[...].astype(F32)
    for side in range(2):
        first = 0 if side == 0 else n - reach

        tap = edge_tap(now, halo, first, reach)

        def emit(j, rows, value):
            x = first + j
            push = speed[x, rows] * value
            kern_out[x, rows] = kern[x, rows] - adj[x, rows] * push
            here = now[x, rows]
            new = ((here + here) - prev[x, rows]) - push
            nxt[x, rows] = new
            if not last:
                (low_out if side == 0 else high_out)[j, rows] = new.astype(BF16)

        stiff_group(tap, first, reach, reach, coef, wz, ly, part, emit)
        if last:
            copies[1 + side].start()
            rows_plane = collect.shape[0]

            def put(j, value):
                at = (side * reach + j) * rows_plane
                edge[at : at + rows_plane] = value

            tile_gradients(lambda j: kern_out[first + j], izt, collect, reach, put)
    if last:
        by = outgoing.shape[1]
        per_plane = collect.shape[0] // by
        alive = live[0]
        zero = jnp.zeros(outgoing.shape[1:], BF16)

        def clear(i, carry):
            outgoing[i] = zero
            return carry

        lax.fori_loop(0, outgoing.shape[0], clear, 0, unroll=8)
        border = reach * per_plane
        middle = (n - 2 * reach) * per_plane

        def move(source, base, count, start):
            def one(i, carry):
                t = start + i
                value = source[pl.ds(pl.multiple_of((base + i) * by, by), by)]
                outgoing[slot[t]] = jnp.where(t < alive, value, zero)
                return carry

            lax.fori_loop(0, count, one, 0, unroll=8)

        move(edge, 0, border, 0)
        move(inner, 0, middle, border)
        move(edge, border, border, border + middle)
        for copy in copies:
            copy.wait()


def gather_body(events, slabs, asked, place, *refs):
    models, pieces = refs[:events], refs[events:]
    count = pieces[0].shape[0]
    share = count // events
    for r, piece in enumerate(pieces):
        base = lax.rem(place[1] + r, slabs) * count
        for k in range(events):

            def one(i, carry, piece=piece, base=base, k=k):
                at = k * share + i
                piece[at] = models[k][asked[base + at]]
                return carry

            lax.fori_loop(0, share, one, 0, unroll=min(8, share))


def reduce_body(events, per_event, ids, place, received, total, *parts):
    for part in parts:
        part[...] = jnp.zeros_like(part)
    here = place[0]
    for source in range(events):
        turn = lax.rem(source - here + events, events)

        def some(i, carry, source=source, turn=turn):
            for j, part in enumerate(parts):
                at = i * len(parts) + j
                row = ids[turn * per_event + at]
                part[row] += received[source * per_event + at].astype(F32)
            return carry

        lax.fori_loop(0, per_event // len(parts), some, 0, unroll=4)
    value = parts[0][...]
    for part in parts[1:]:
        value = value + part[...]
    total[...] = value


def shards(
    wave_prev,
    wave_now,
    adjoint,
    background,
    coeffs_x,
    stiff_y,
    stiff_z,
    interp_y,
    interp_z,
    model,
    block_index,
    live_count,
):
    n_event = lax.axis_size("event")
    n_slab = lax.axis_size("slab")
    devices = n_event * n_slab
    event = lax.axis_index("event")
    slab = lax.axis_index("slab")
    blk_dev, by, bz = model.shape
    n_planes, ny, nz = wave_now.shape[1:]
    per_plane = block_index.shape[2]
    n_tiles = n_planes * per_plane
    capacity = max(1, 2 * n_tiles // devices)
    n_steps = adjoint.shape[1]
    taps = coeffs_x.shape[-1]
    reach = (taps - 1) // 2
    per_event = n_slab * capacity
    slots = n_event * per_event

    models = [model]
    for k in range(1, n_event):
        models.append(lax.ppermute(model, "event", [(i, (i + k) % n_event) for i in range(n_event)]))

    ids = block_index[0].reshape(n_tiles)
    owner = ids // blk_dev
    local = ids % blk_dev
    order = jnp.arange(n_tiles, dtype=I32)
    same = (owner[:, None] == owner[None, :]) & (order[None, :] < order[:, None])
    rank = jnp.sum(same.astype(I32), axis=1)
    turn = (event - owner // n_slab + n_event) % n_event
    share = n_event * capacity
    within = turn * capacity + rank
    slot_ask = (owner % n_slab) * share + within
    slot_fetch = ((slab - owner % n_slab + n_slab) % n_slab) * share + within
    slot_send = owner * capacity + rank
    hit = slot_ask[None, :] == jnp.arange(slots, dtype=I32)[:, None]
    requests = jnp.sum(jnp.where(hit, local[None, :], 0), axis=1).reshape(n_slab, share)
    tile = 8 * 128
    padded = -(-share // tile) * tile
    requests = jnp.pad(requests, ((0, 0), (0, padded - share))).reshape(n_slab, padded // 128, 128)
    asked = lax.all_to_all(requests, "slab", split_axis=0, concat_axis=0, tiled=True)
    asked = asked.reshape(n_slab, padded)[:, :share]
    place = jnp.stack([event, slab]).astype(I32)
    pieces = call(
        functools.partial(gather_body, n_event, n_slab),
        [asked.reshape(slots), place] + models,
        [sspec()] * 2 + [vspec()] * n_event,
        [VM((share, by, bz), BF16)] * n_slab,
        mib=4,
        name="gather",
    )
    fetched = [pieces[0]]
    for r in range(1, n_slab):
        fetched.append(lax.ppermute(pieces[r], "slab", [(i, (i + r) % n_slab) for i in range(n_slab)]))

    asked_turn = asked.reshape(n_slab, n_event, capacity).transpose(1, 0, 2).reshape(n_event, per_event)
    row_ids = [asked_turn[0]]
    for k in range(1, n_event):
        row_ids.append(
            lax.ppermute(asked_turn[k], "event", [(i, (i - k) % n_event) for i in range(n_event)])
        )
    row_ids = jnp.concatenate(row_ids)

    szh, szl = split2_outside(stiff_z.T)
    wz = jnp.concatenate(
        [jnp.concatenate([szh, szl], axis=1), jnp.concatenate([szh, jnp.zeros_like(szl)], axis=1)], axis=0
    )
    syh, syl = split2_outside(stiff_y)
    ly = jnp.concatenate(
        [jnp.concatenate([syh, syh], axis=1), jnp.concatenate([syl, jnp.zeros_like(syl)], axis=1)], axis=0
    )
    eye = jnp.eye(per_plane, dtype=BF16)
    spread = jnp.einsum("qp,br->qrpb", eye, interp_y).reshape(ny, per_plane * by)
    collect = jnp.concatenate([spread.T, spread.T], axis=1)
    spread = jnp.concatenate([spread, spread], axis=1)
    izt = interp_z.T
    coef = coeffs_x[0].reshape(n_planes * taps)
    live = live_count.reshape(1)

    up = [(i, i + 1) for i in range(n_slab - 1)]
    down = [(j, i) for i, j in up]

    def exchange(low, high):
        return lax.ppermute(high, "slab", up), lax.ppermute(low, "slab", down)

    cube = (n_planes, ny, nz)
    part = VM((reach, ny, nz), F32)
    below, above = exchange(wave_now[0, :reach].astype(BF16), wave_now[0, n_planes - reach :].astype(BF16))
    stiff, ahead, now, back, *adj = call(
        functools.partial(first_body, reach, n_steps),
        [hbm(a) for a in (wave_now, wave_prev, background, adjoint)] + [below, above, coef, wz, ly, spread, collect, izt],
        [aspec()] * 4 + [vspec()] * 2 + [sspec()] + [vspec()] * 5,
        [VM(cube, F32)] * (4 + n_steps),
        [VM(cube, F32), VM((2 * reach, ny, nz), F32), part, pltpu.SemaphoreType.DMA((3 + n_steps,))],
        mib=8,
        name="first",
    )
    adj = [in_vmem(a) for a in adj]
    edges = [jax.ShapeDtypeStruct((reach, ny, nz), BF16)] * 2
    speed, nxt, kern, low, high = call(
        functools.partial(start_body, reach, n_slab),
        [in_vmem(f) for f in fetched]
        + [slot_fetch, live, interp_z, spread, in_vmem(back), in_vmem(ahead), in_vmem(stiff), adj[0]],
        [vspec()] * n_slab + [sspec()] * 2 + [vspec()] * 6,
        [VM(cube, F32), VM(cube, F32), VM(cube, F32)] + edges,
        [VM((slots, by, bz), BF16), VM((n_tiles * by, bz), BF16), VM((n_tiles * by, nz), F32)],
        aliases={n_slab + 5: 1, n_slab + 6: 2},
        mib=6,
        name="start",
    )
    prev, now = now, nxt
    for s in range(1, n_steps):
        last = s == n_steps - 1
        below, above = exchange(low, high)
        inputs = [in_vmem(now), in_vmem(prev), in_vmem(speed), in_vmem(kern), adj[s]]
        specs = [vspec()] * 5
        more = [izt, collect] if last else []
        outs = [VM(cube, F32), VM(cube, F32)]
        rows_inner = (n_planes - 2 * reach) * per_plane * by
        result = call(
            functools.partial(inner_body, reach, last),
            inputs + [coef, wz, ly] + more,
            specs + [sspec()] + [vspec()] * (2 + len(more)),
            outs + ([VM((rows_inner, bz), BF16)] if last else []),
            [part],
            aliases={1: 0, 3: 1},
            mib=4,
            name="inner",
        )
        mid, kern = result[:2]
        if last:
            more = [izt, collect, in_vmem(result[2]), slot_send, live]
            more_specs = [vspec()] * 3 + [sspec()] * 2
            more_outs = [
                jax.ShapeDtypeStruct((slots, by, bz), BF16),
                jax.ShapeDtypeStruct((1,) + cube, F32),
            ]
            more_scratch = [VM((2 * reach * per_plane * by, bz), BF16), pltpu.SemaphoreType.DMA((3,))]
        else:
            more, more_specs, more_outs, more_scratch = [], [], edges, []
        result = call(
            functools.partial(outer_body, reach, last),
            [in_vmem(now), in_vmem(mid), in_vmem(speed), in_vmem(kern), adj[s], below, above, coef, wz, ly] + more,
            specs + [vspec()] * 2 + [sspec()] + [vspec()] * 2 + more_specs,
            outs + more_outs,
            [part, VM((2 * reach, ny, nz), F32)] + more_scratch,
            aliases={1: 0, 3: 1},
            mib=6,
            name="outer",
            out_specs=[vspec()] * (2 + len(more_outs)) if not last else [vspec()] * 3 + [aspec()],
        )
        nxt, kern = result[:2]
        if last:
            outgoing, wave_last = result[2:]
        else:
            low, high = result[2:]
        prev, now = now, nxt
    received = lax.all_to_all(
        outgoing.reshape(devices, capacity, by, bz), ("event", "slab"), split_axis=0, concat_axis=0, tiled=True
    ).reshape(slots, by, bz)
    gradient = call(
        functools.partial(reduce_body, n_event, per_event),
        [row_ids, place, received],
        [sspec(), sspec(), vspec()],
        [jax.ShapeDtypeStruct((blk_dev, by, bz), F32)],
        [VM((blk_dev, by, bz), F32)] * 4,
        mib=8,
        name="reduce",
    )[0]
    return (wave_last, gradient)


def solution(mesh):
    return jax.shard_map(
        shards,
        mesh=mesh,
        in_specs=(
            P("event", "slab", None, None),
            P("event", "slab", None, None),
            P("event", None, "slab", None, None),
            P("event", "slab", None, None),
            P("event", "slab", None),
            P(),
            P(),
            P(),
            P(),
            P(("event", "slab"), None, None),
            P("event", "slab", None),
            P("event", "slab"),
        ),
        out_specs=(P("event", "slab", None, None), P(("event", "slab"), None, None)),
        check_vma=False,
    )
```

```python
import functools

import jax
import jax.numpy as jnp
from jax import lax
from jax.experimental import pallas as pl
from jax.experimental.pallas import tpu as pltpu
from jax.sharding import PartitionSpec as P


F32 = jnp.float32
BF16 = jnp.bfloat16
I32 = jnp.int32
VM = pltpu.VMEM
ROWS = 32


def vspec():
    return pl.BlockSpec(memory_space=pltpu.VMEM)


def sspec():
    return pl.BlockSpec(memory_space=pltpu.SMEM)


def aspec():
    return pl.BlockSpec(memory_space=pl.ANY)


def in_vmem(x):
    return pltpu.with_memory_space_constraint(x, pltpu.VMEM)


def hbm(x):
    return pltpu.with_memory_space_constraint(x, pltpu.HBM)


def split2(value):
    high = value.astype(BF16)
    low = (value - high.astype(F32)).astype(BF16)
    return high, low


def split2_outside(value):
    rounded = lax.reduce_precision(value, exponent_bits=8, mantissa_bits=7)
    return rounded.astype(BF16), (value - rounded).astype(BF16)


def call(body, args, specs, outs, scratch=(), aliases=None, mib=24, out_specs=None):
    return pl.pallas_call(
        body,
        out_shape=outs,
        in_specs=specs,
        out_specs=out_specs or [vspec() for _ in outs],
        scratch_shapes=list(scratch),
        input_output_aliases=aliases or {},
        compiler_params=pltpu.CompilerParams(vmem_limit_bytes=mib * 1024 * 1024),
    )(*args)


def partner(index, turn, size):
    if size & (size - 1) == 0:
        return index ^ turn
    return (index + turn) % size


def turn_from(here, source, size):
    if size & (size - 1) == 0:
        return here ^ source
    return (here - source + size) % size


def far_first(size):
    return sorted(range(1, size), key=lambda r: (-bin(r >> 1).count("1"), r & 1, r))


def both_ways(ring, size, back=False):
    pairs = [(i, partner(i, ring, size)) for i in range(size)]
    return [(j, i) for i, j in pairs] if back else pairs


def hand_out(even, sides, near, far):
    @pl.when(even)
    def _():
        near[...] = sides[1]
        far[...] = sides[0]

    @pl.when(jnp.logical_not(even))
    def _():
        near[...] = sides[0]
        far[...] = sides[1]


def take_in(even, halo, near, far, reach, ny):
    @pl.when(even)
    def _():
        halo[0:reach, 0:ny] = far[...].astype(F32)
        halo[reach : 2 * reach, 0:ny] = near[...].astype(F32)

    @pl.when(jnp.logical_not(even))
    def _():
        halo[0:reach, 0:ny] = near[...].astype(F32)
        halo[reach : 2 * reach, 0:ny] = far[...].astype(F32)


def is_even(place):
    return lax.rem(place[1], 2) == 0


def along_planes(tap, width, reach, wz, ly, part):
    ny, nz = part.shape[1:]
    every = slice(0, ny)
    for j in range(0, width, 2):
        ah, al = split2(tap(reach + j)(every))
        bh, bl = split2(tap(reach + j + 1)(every))
        left = jnp.concatenate(
            [jnp.concatenate([ah, al], axis=1), jnp.concatenate([bh, bl], axis=1)], axis=0
        )
        rz = jnp.dot(left, wz[...], preferred_element_type=F32)
        right = jnp.concatenate(
            [jnp.concatenate([ah, bh], axis=1), jnp.concatenate([al, bl], axis=1)], axis=0
        )
        ry = jnp.dot(ly[...], right, preferred_element_type=F32)
        part[j] = (rz[:ny, :nz] + rz[:ny, nz:]) + (ry[:ny, :nz] + ry[ny:, :nz])
        part[j + 1] = (rz[ny:, :nz] + rz[ny:, nz:]) + (ry[:ny, nz:] + ry[ny:, nz:])


def across_planes(tap, first, width, reach, coef, part, emit):
    taps = 2 * reach + 1
    for j in range(width):
        weights = [coef[(first + j) * taps + k] for k in range(taps)]
        for row in range(0, part.shape[1], ROWS):
            rows = slice(row, row + ROWS)
            total = part[j, rows]
            for k in range(taps):
                total = total + weights[k] * tap(j + k)(rows)
            emit(j, rows, total)


def stiff_groups(firsts, taps, reach, coef, wz, ly, part, emits):
    for i, tap in enumerate(taps):
        along_planes(tap, reach, reach, wz, ly, part.at[pl.ds(i * reach, reach)])
    for i, (first, tap, emit) in enumerate(zip(firsts, taps, emits)):
        across_planes(tap, first, reach, reach, coef, part.at[pl.ds(i * reach, reach)], emit)


def inside(now, reach, first):
    return lambda j: lambda rows: now[first - reach + j, rows]


def border_body(reach, wave, place, near, far, planes, sides, sems):
    n = wave.shape[1]
    copies = [
        pltpu.make_async_copy(wave.at[0, pl.ds(at, reach)], planes.at[i], sems.at[i])
        for i, at in enumerate((0, n - reach))
    ]
    for copy in copies:
        copy.start()
    for copy in copies:
        copy.wait()
    sides[...] = planes[...].astype(BF16)
    hand_out(is_even(place), sides, near, far)


def first_body(reach, *refs):
    wave, before, back, adjoint, near, far, place, coef, wz, ly = refs[:10]
    refs = refs[13:]
    stiff, ahead, now, background, adj, prev, halo, part, sems = refs
    n, ny = stiff.shape[:2]
    rows = pl.ds(0, ny)
    lump = 2 * reach

    def arrival(i):
        at = pl.ds(i * lump, lump)
        return (
            pltpu.make_async_copy(wave.at[0, at], now.at[at, rows], sems.at[0, i]),
            pltpu.make_async_copy(before.at[0, at], prev.at[at], sems.at[1, i]),
        )

    for i in range(n // lump):
        for copy in arrival(i):
            copy.start()
    copies = [
        pltpu.make_async_copy(back.at[0], background, sems.at[2, 0]),
        pltpu.make_async_copy(adjoint.at[0, 0], adj, sems.at[3, 0]),
    ]
    for copy in copies:
        copy.start()
    take_in(is_even(place), halo, near, far, reach, ny)
    for copy in arrival(0):
        copy.wait()

    def emit_at(first):
        def emit(j, rows, value):
            stiff[first + j, rows] = value
            here = now[first + j, rows]
            ahead[first + j, rows] = (here + here) - prev[first + j, rows]

        return emit

    def groups(firsts, taps):
        stiff_groups(firsts, taps, reach, coef, wz, ly, part, [emit_at(first) for first in firsts])

    def step(i, carry):
        for copy in arrival(i + 1):
            copy.wait()
        firsts = [(2 * i + 1) * reach, (2 * i + 2) * reach]
        groups(firsts, [inside(now, reach, first) for first in firsts])
        return carry

    lax.fori_loop(0, n // lump - 1, step, 0)
    firsts = [0, n - reach]
    groups(firsts, [edge_tap(now, halo, first, reach) for first in firsts])
    for copy in copies:
        copy.wait()


def edge_tap(now, halo, first, reach):
    n = now.shape[0]

    def tap(j):
        x = first - reach + j
        if x < 0:
            return lambda rows: halo[j, rows]
        if x >= n:
            return lambda rows: halo[reach + x - n, rows]
        return lambda rows: now[x, rows]

    return tap


def start_body(reach, slabs, *refs):
    fetched, refs = refs[:slabs], refs[slabs:]
    slot, live, place, iz, spread, background, ahead, stiff, adj, adjoint = refs[:10]
    speed, nxt, kern, near, far, adj_next, table, blocks, along, sides, sems = refs[10:]
    copy = pltpu.make_async_copy(adjoint.at[0, 1], adj_next, sems.at[0])
    copy.start()
    n, ny, nz = background.shape
    tiles = slot.shape[0]
    per_plane = tiles // n
    by = table.shape[1]
    rows_plane = per_plane * by
    alive = live[0]
    zero = jnp.zeros(table.shape[1:], BF16)
    count = fetched[0].shape[0]
    for r, piece in enumerate(fetched):
        table[r * count : (r + 1) * count] = piece[...]

    def lay(t, carry):
        block = table[slot[t]]
        blocks[pl.ds(pl.multiple_of(t * by, by), by)] = jnp.where(t < alive, block, zero)
        return carry

    lax.fori_loop(0, tiles, lay, 0, unroll=8)
    chunk = 8 * rows_plane

    def group(g, carry):
        at = pl.ds(pl.multiple_of(g * chunk, chunk), chunk)
        along[...] = jnp.dot(blocks[at], iz[...], preferred_element_type=F32)
        for i in range(0, 8, 2):
            cols = []
            for j in (i, i + 1):
                high, low = split2(along[j * rows_plane : (j + 1) * rows_plane])
                cols.append(jnp.concatenate([high, low], axis=0))
            perturb = jnp.dot(spread[...], jnp.concatenate(cols, axis=1), preferred_element_type=F32)
            for j in range(2):
                x = 8 * g + i + j
                c = background[x] * jnp.exp(perturb[:, j * nz : (j + 1) * nz])
                speed[x] = c
                push = c * stiff[x]
                nxt[x, 0:ny] = ahead[x, 0:ny] - push
                kern[x] = -(adj[x] * push)
        return carry

    lax.fori_loop(0, n // 8, group, 0)
    sides[0] = nxt[0:reach, 0:ny].astype(BF16)
    sides[1] = nxt[n - reach : n, 0:ny].astype(BF16)
    hand_out(is_even(place), sides, near, far)
    copy.wait()


def tile_gradients(kern_plane, izt, collect, width, put):
    for j in range(0, width, 2):
        cols = []
        for i in (j, j + 1):
            back = jnp.dot(kern_plane(i).astype(BF16), izt[...], preferred_element_type=F32)
            high, low = split2(back)
            cols.append(jnp.concatenate([high, low], axis=0))
        grads = jnp.dot(collect[...], jnp.concatenate(cols, axis=1), preferred_element_type=F32)
        half = grads.shape[1] // 2
        put(j, grads[:, :half].astype(BF16))
        put(j + 1, grads[:, half:].astype(BF16))


def send_tiles(source, base, count, start, slot, live, outgoing):
    by = outgoing.shape[1]
    alive = live[0]
    zero = jnp.zeros(outgoing.shape[1:], BF16)

    def one(i, carry):
        t = start + i
        value = source[pl.ds(pl.multiple_of((base + i) * by, by), by)]
        outgoing[slot[t]] = jnp.where(t < alive, value, zero)
        return carry

    lax.fori_loop(0, count, one, 0, unroll=8)


def inner_body(reach, step_at, last, now, prev, speed, kern, adj, coef, wz, ly, *rest):
    if last:
        izt, collect, slot, live, nxt, kern_out, outgoing, part, inner = rest
        zero = jnp.zeros(outgoing.shape[1:], BF16)

        def clear(i, carry):
            outgoing[i] = zero
            return carry

        lax.fori_loop(0, outgoing.shape[0], clear, 0, unroll=8)
    else:
        adjoint, nxt, kern_out, adj_next, part, sems = rest
        copy = pltpu.make_async_copy(adjoint.at[0, step_at + 1], adj_next, sems.at[0])
        copy.start()
    n = speed.shape[0]

    def emit_at(first):
        def emit(j, rows, value):
            x = first + j
            push = speed[x, rows] * value
            kern_out[x, rows] = kern[x, rows] - adj[x, rows] * push
            here = now[x, rows]
            nxt[x, rows] = ((here + here) - prev[x, rows]) - push

        return emit

    groups = n // reach - 2
    lot = part.shape[0] // reach

    def step(i, carry):
        firsts = [(lot * i + 1 + q) * reach for q in range(lot)]
        stiff_groups(
            firsts,
            [inside(now, reach, first) for first in firsts],
            reach, coef, wz, ly, part,
            [emit_at(first) for first in firsts],
        )
        if last:
            rows_plane = collect.shape[0]

            def put(j, value):
                at = pl.multiple_of((lot * reach * i + j) * rows_plane, rows_plane)
                inner[pl.ds(at, rows_plane)] = value

            tile_gradients(lambda j: kern_out[firsts[0] + j], izt, collect, lot * reach, put)
        return carry

    lax.fori_loop(0, groups // lot, step, 0)
    if last:
        per_plane = collect.shape[0] // outgoing.shape[1]
        send_tiles(inner, 0, (n - 2 * reach) * per_plane, reach * per_plane, slot, live, outgoing)
    else:
        copy.wait()


def outer_body(reach, last, now, prev, speed, kern, adj, near, far, place, coef, wz, ly, *rest):
    if last:
        izt, collect, slot, live, inner, nxt, kern_out, outgoing, wave, part, halo, edge, sems = rest
    else:
        nxt, kern_out, near_out, far_out, part, halo, sides = rest
    n, ny = speed.shape[:2]
    even = is_even(place)
    if last:
        every = pl.ds(0, ny)
        copies = [
            pltpu.make_async_copy(nxt.at[pl.ds(at, count), every], wave.at[0, pl.ds(at, count)], sems.at[i])
            for i, (at, count) in enumerate([(reach, n - 2 * reach), (0, reach), (n - reach, reach)])
        ]
        copies.append(pltpu.make_async_copy(inner, outgoing, sems.at[3]))
        copies[0].start()
        copies[3].start()
    take_in(even, halo, near, far, reach, ny)

    def emit_at(side, first):
        def emit(j, rows, value):
            x = first + j
            push = speed[x, rows] * value
            kern_out[x, rows] = kern[x, rows] - adj[x, rows] * push
            here = now[x, rows]
            new = ((here + here) - prev[x, rows]) - push
            nxt[x, rows] = new
            if not last:
                sides[side, j, rows] = new.astype(BF16)

        return emit

    firsts = [0, n - reach]
    stiff_groups(
        firsts,
        [edge_tap(now, halo, first, reach) for first in firsts],
        reach, coef, wz, ly, part,
        [emit_at(side, first) for side, first in enumerate(firsts)],
    )
    if last:
        copies[1].start()
        copies[2].start()
        by, bz = edge.shape[1:]
        per_plane = collect.shape[0] // by

        def put(j, value):
            edge[j * per_plane : (j + 1) * per_plane] = value.reshape(per_plane, by, bz)

        def border_plane(j):
            return kern_out[j if j < reach else n - 2 * reach + j]

        tile_gradients(border_plane, izt, collect, 2 * reach, put)
    if last:
        border = reach * per_plane
        alive = live[0]
        zero = jnp.zeros((by, bz), BF16)
        copies.pop().wait()
        for side in range(2):

            def one(i, carry):
                at = side * border + i
                t = i if side == 0 else (n - reach) * per_plane + i
                edge[at] = jnp.where(t < alive, edge[at], zero)
                pltpu.make_async_copy(edge.at[at], outgoing.at[slot[t]], sems.at[4]).start()
                return carry

            lax.fori_loop(0, border, one, 0, unroll=4)
        pltpu.make_async_copy(edge, edge, sems.at[4]).wait()
        for copy in copies:
            copy.wait()
    else:
        hand_out(even, sides, near_out, far_out)


def gather_body(events, slabs, asked, place, *refs):
    models, pieces = refs[:events], refs[events:]
    count = pieces[0].shape[0]
    share = count // events
    for r, piece in enumerate(pieces):
        base = partner(place[1], r, slabs) * count
        for k in range(events):

            def one(i, carry, piece=piece, base=base, k=k):
                at = k * share + i
                piece[at] = models[k][asked[base + at]]
                return carry

            lax.fori_loop(0, share, one, 0, unroll=min(8, share))


def reduce_body(events, per_event, ids, place, received, total, *parts):
    for part in parts:
        part[...] = jnp.zeros_like(part)
    here = place[0]
    for source in range(events):
        turn = turn_from(source, here, events)

        def some(i, carry, source=source, turn=turn):
            for j, part in enumerate(parts):
                at = i * len(parts) + j
                row = ids[turn * per_event + at]
                part[row] += received[source * per_event + at].astype(F32)
            return carry

        lax.fori_loop(0, per_event // len(parts), some, 0, unroll=4)
    value = parts[0][...]
    for part in parts[1:]:
        value = value + part[...]
    total[...] = value


def shards(
    wave_prev,
    wave_now,
    adjoint,
    background,
    coeffs_x,
    stiff_y,
    stiff_z,
    interp_y,
    interp_z,
    model,
    block_index,
    live_count,
):
    n_event = lax.axis_size("event")
    n_slab = lax.axis_size("slab")
    devices = n_event * n_slab
    event = lax.axis_index("event")
    slab = lax.axis_index("slab")
    blk_dev, by, bz = model.shape
    n_planes, ny, nz = wave_now.shape[1:]
    per_plane = block_index.shape[2]
    n_tiles = n_planes * per_plane
    capacity = max(1, 2 * n_tiles // devices)
    n_steps = adjoint.shape[1]
    taps = coeffs_x.shape[-1]
    reach = (taps - 1) // 2
    per_event = n_slab * capacity
    slots = n_event * per_event

    models = [model] + [None] * (n_event - 1)
    for k in far_first(n_event):
        models[k] = lax.ppermute(model, "event", both_ways(k, n_event))

    ids = block_index[0].reshape(n_tiles)
    owner = ids // blk_dev
    local = ids % blk_dev
    order = jnp.arange(n_tiles, dtype=I32)
    same = (owner[:, None] == owner[None, :]) & (order[None, :] < order[:, None])
    rank = jnp.sum(same.astype(I32), axis=1)
    turn = turn_from(event, owner // n_slab, n_event)
    share = n_event * capacity
    within = turn * capacity + rank
    slot_ask = (owner % n_slab) * share + within
    slot_fetch = turn_from(slab, owner % n_slab, n_slab) * share + within
    slot_send = owner * capacity + rank
    hit = slot_ask[None, :] == jnp.arange(slots, dtype=I32)[:, None]
    requests = jnp.sum(jnp.where(hit, local[None, :], 0), axis=1).reshape(n_slab, share)
    tile = 8 * 128
    padded = -(-share // tile) * tile
    requests = jnp.pad(requests, ((0, 0), (0, padded - share))).reshape(n_slab, padded // 128, 128)
    asked = lax.all_to_all(requests, "slab", split_axis=0, concat_axis=0, tiled=True)
    asked = asked.reshape(n_slab, padded)[:, :share]
    place = jnp.stack([event, slab]).astype(I32)
    pieces = call(
        functools.partial(gather_body, n_event, n_slab),
        [asked.reshape(slots), place] + models,
        [sspec()] * 2 + [vspec()] * n_event,
        [VM((share, by, bz), BF16)] * n_slab,
        mib=4,
    )
    fetched = [pieces[0]] + [None] * (n_slab - 1)
    for r in far_first(n_slab):
        fetched[r] = lax.ppermute(pieces[r], "slab", both_ways(r, n_slab))

    asked_turn = asked.reshape(n_slab, n_event, capacity).transpose(1, 0, 2).reshape(n_event, per_event)
    row_ids = [asked_turn[0]]
    for k in range(1, n_event):
        row_ids.append(lax.ppermute(asked_turn[k], "event", both_ways(k, n_event, back=True)))
    row_ids = jnp.concatenate(row_ids)

    szh, szl = split2_outside(stiff_z.T)
    wz = jnp.concatenate(
        [jnp.concatenate([szh, szl], axis=1), jnp.concatenate([szh, jnp.zeros_like(szl)], axis=1)], axis=0
    )
    syh, syl = split2_outside(stiff_y)
    ly = jnp.concatenate(
        [jnp.concatenate([syh, syh], axis=1), jnp.concatenate([syl, jnp.zeros_like(syl)], axis=1)], axis=0
    )
    eye = jnp.eye(per_plane, dtype=BF16)
    spread = jnp.einsum("qp,br->qrpb", eye, interp_y).reshape(ny, per_plane * by)
    collect = jnp.concatenate([spread.T, spread.T], axis=1)
    spread = jnp.concatenate([spread, spread], axis=1)
    izt = interp_z.T
    coef = coeffs_x[0].reshape(n_planes * taps)
    live = live_count.reshape(1)

    near_pairs = [(i, i ^ 1) for i in range(n_slab) if i ^ 1 < n_slab]
    far_pairs = [(i, i + 1) for i in range(1, n_slab - 1, 2)]
    far_pairs = far_pairs + [(j, i) for i, j in far_pairs]

    def exchange(near, far):
        far = lax.ppermute(far, "slab", far_pairs)
        near = lax.ppermute(near, "slab", near_pairs)
        return near, far

    cube = (n_planes, ny, nz)
    halo = VM((2 * reach, ny, nz), F32)
    part = VM((2 * reach, ny, nz), F32)
    sides = VM((2, reach, ny, nz), BF16)
    lot = next(q for q in (3, 2, 1) if (n_planes // reach - 2) % q == 0)
    edges = [VM((reach, ny, nz), BF16)] * 2
    dma = pltpu.SemaphoreType.DMA
    near, far = call(
        functools.partial(border_body, reach),
        [hbm(wave_now), place],
        [aspec(), sspec()],
        edges,
        [VM((2, reach, ny, nz), F32), sides, dma((2,))],
        mib=4,
    )
    near, far = exchange(near, far)
    adjoint = hbm(adjoint)
    stiff, ahead, now, back, adj = call(
        functools.partial(first_body, reach),
        [hbm(wave_now), hbm(wave_prev), hbm(background), adjoint]
        + [near, far, place, coef, wz, ly, spread, collect, izt],
        [aspec()] * 4 + [vspec()] * 2 + [sspec()] * 2 + [vspec()] * 5,
        [VM(cube, F32), VM(cube, F32), VM(cube, F32), VM(cube, F32), VM(cube, F32)],
        [VM(cube, F32), halo, part, dma((4, n_planes // (2 * reach)))],
        mib=8,
    )
    speed, nxt, kern, near, far, adj_next = call(
        functools.partial(start_body, reach, n_slab),
        [in_vmem(f) for f in fetched]
        + [slot_fetch, live, place, interp_z, spread]
        + [in_vmem(a) for a in (back, ahead, stiff, adj)]
        + [adjoint],
        [vspec()] * n_slab + [sspec()] * 3 + [vspec()] * 6 + [aspec()],
        [VM(cube, F32), VM(cube, F32), VM(cube, F32)] + edges + [VM(cube, F32)],
        [VM((slots, by, bz), BF16), VM((n_tiles * by, bz), BF16), VM((8 * per_plane * by, nz), F32), sides, dma((1,))],
        aliases={n_slab + 6: 1, n_slab + 7: 2},
        mib=6,
    )
    prev, now, adj = now, nxt, adj_next
    for s in range(1, n_steps):
        last = s == n_steps - 1
        near, far = exchange(near, far)
        specs = [vspec()] * 5
        if last:
            more, more_specs = [izt, collect, slot_send, live], [vspec()] * 2 + [sspec()] * 2
            more_outs = [VM((slots, by, bz), BF16)]
            more_scratch = [VM(((n_planes - 2 * reach) * per_plane * by, bz), BF16)]
        else:
            more, more_specs = [adjoint], [aspec()]
            more_outs = [VM(cube, F32)]
            more_scratch = [dma((1,))]
        mid, kern, extra = call(
            functools.partial(inner_body, reach, s, last),
            [in_vmem(a) for a in (now, prev, speed, kern, adj)] + [coef, wz, ly] + more,
            specs + [sspec()] + [vspec()] * 2 + more_specs,
            [VM(cube, F32), VM(cube, F32)] + more_outs,
            [VM((lot * reach, ny, nz), F32)] + more_scratch,
            aliases={1: 0, 3: 1},
            mib=6,
        )
        if last:
            more, more_specs = more + [in_vmem(extra)], more_specs + [vspec()]
            more_outs = [pltpu.HBM((slots, by, bz), BF16), pltpu.HBM((1,) + cube, F32)]
            more_scratch = [VM((2 * reach * per_plane, by, bz), BF16), dma((5,))]
        else:
            more, more_specs, more_outs, more_scratch = [], [], edges, [sides]
        nxt, kern, *result = call(
            functools.partial(outer_body, reach, last),
            [in_vmem(a) for a in (now, mid, speed, kern, adj)] + [near, far, place, coef, wz, ly] + more,
            specs + [vspec()] * 2 + [sspec()] * 2 + [vspec()] * 2 + more_specs,
            [VM(cube, F32), VM(cube, F32)] + more_outs,
            [part, halo] + more_scratch,
            aliases={1: 0, 3: 1},
            mib=6,
            out_specs=[vspec()] * 2 + [aspec()] * 2 if last else None,
        )
        if last:
            outgoing, wave_last = result
        else:
            near, far = result
        prev, now, adj = now, nxt, extra
    received = lax.all_to_all(
        outgoing.reshape(devices, capacity, by, bz), ("event", "slab"), split_axis=0, concat_axis=0, tiled=True
    ).reshape(slots, by, bz)
    gradient = call(
        functools.partial(reduce_body, n_event, per_event),
        [row_ids, place, received],
        [sspec(), sspec(), vspec()],
        [jax.ShapeDtypeStruct((blk_dev, by, bz), F32)],
        [VM((blk_dev, by, bz), F32)] * 4,
        mib=8,
    )[0]
    return (wave_last, gradient)


def solution(mesh):
    return jax.shard_map(
        shards,
        mesh=mesh,
        in_specs=(
            P("event", "slab", None, None),
            P("event", "slab", None, None),
            P("event", None, "slab", None, None),
            P("event", "slab", None, None),
            P("event", "slab", None),
            P(),
            P(),
            P(),
            P(),
            P(("event", "slab"), None, None),
            P("event", "slab", None),
            P("event", "slab"),
        ),
        out_specs=(P("event", "slab", None, None), P(("event", "slab"), None, None)),
        check_vma=False,
    )
```
